32 devices in a mesh: dp: 1 (over z), emb: 4 (over y), head: 8 (over x, core).
Axes of the slice: x: 4, y: 4, z: 1, core: 2. Of those that a mesh axis runs over, the one named last changes fastest.
The devices are a block of a 4x4x8 slice.
Arguments:
- hidden: bfloat16 [32, 256, 6144], P('dp', None, 'emb')
- g_in: bfloat16 [6144], P('emb')
- w_dq: bfloat16 [6144, 1536], P('emb', 'head')
- g_q: bfloat16 [1536], P('head')
- w_dkv: bfloat16 [6144, 512], P('emb', 'head')
- g_kv: bfloat16 [512], P('head')
- w_kr: bfloat16 [6144, 64], P('emb')
- w_uq: bfloat16 [1536, 64, 192], P(None, 'head')
- w_uk: bfloat16 [512, 64, 128], P(None, 'head')
- w_uv: bfloat16 [512, 64, 128], P(None, 'head')
- w_o: bfloat16 [64, 128, 6144], P('head', None, 'emb')
Outputs:
- output 1: bfloat16 [32, 256, 6144], P('dp', None, 'emb')
- output 2: bfloat16 [32, 256, 512], P('dp', None, 'head')
- output 3: bfloat16 [32, 256, 64], P('dp')
All inputs are finite; a program needn't handle non-finite values.
Results may differ from the reference program's by a relative error of at most 0.02.
Values are sent between devices in bfloat16 or wider.
A program may use at most 768 MiB of HBM per device.

```python
import math
import jax
import jax.numpy as jnp
from jax import lax

BATCH = 32
SEQ = 256
D = 6144
HEADS = 64
Q_LORA = 1536
KV_LORA = 512
NOPE = 128
ROPE = 64
VDIM = 128

QK_DIM = NOPE + ROPE
HALF_ROPE = ROPE // 2
Q_BLOCK = min(SEQ, 128)
BLOCKS_PER_SEQ = SEQ // Q_BLOCK
NUM_BLOCKS = BATCH * BLOCKS_PER_SEQ
ROPE_BASE = 10000.0
NORM_EPS = 1.0e-6
MSCALE = 0.1 * math.log(40.0) + 1.0
SOFTMAX_SCALE = MSCALE * MSCALE / math.sqrt(QK_DIM)


def setup_inputs(seed: int = 0, part: int = 0) -> dict:
    key_list = jax.random.split(jax.random.key(seed), 10)
    part_key = jax.random.fold_in(jax.random.key(seed + 1), part)

    def make_gain(sub_key, count):
        return jax.random.uniform(sub_key, (count,), jnp.float32, 0.5, 1.5).astype(jnp.bfloat16)

    def weight(sub_key, arr_shape, fan_in):
        return (jax.random.normal(sub_key, arr_shape, jnp.float32) * fan_in ** -0.5).astype(jnp.bfloat16)

    hidden = 0.5 * jax.random.normal(part_key, (BATCH, SEQ, D), jnp.float32)
    return {
        "hidden": hidden.astype(jnp.bfloat16),
        "g_in": make_gain(key_list[0], D),
        "w_dq": weight(key_list[1], (D, Q_LORA), D),
        "g_q": make_gain(key_list[2], Q_LORA),
        "w_dkv": weight(key_list[3], (D, KV_LORA), D),
        "g_kv": make_gain(key_list[4], KV_LORA),
        "w_kr": weight(key_list[5], (D, ROPE), D),
        "w_uq": weight(key_list[6], (Q_LORA, HEADS, QK_DIM), Q_LORA),
        "w_uk": weight(key_list[7], (KV_LORA, HEADS, NOPE), KV_LORA),
        "w_uv": weight(key_list[8], (KV_LORA, HEADS, VDIM), KV_LORA),
        "w_o": weight(key_list[9], (HEADS, VDIM, D), HEADS * VDIM),
    }


def rms_norm(values, gain_vec):
    wide_vals = values.astype(jnp.float32)
    mean_sq = jnp.mean(wide_vals * wide_vals, axis=-1, keepdims=True)
    return (wide_vals * lax.rsqrt(mean_sq + NORM_EPS) * gain_vec.astype(jnp.float32)).astype(jnp.bfloat16)


def rope_tables():
    inv_freq = ROPE_BASE ** (-2.0 * jnp.arange(HALF_ROPE, dtype=jnp.float32) / ROPE)
    angles = jnp.arange(SEQ, dtype=jnp.float32)[:, None] * inv_freq[None, :]
    return jnp.cos(angles), jnp.sin(angles)


def rotate(values, cos_t, sin_t):
    front_half = values[..., :HALF_ROPE]
    back_half = values[..., HALF_ROPE:]
    return jnp.concatenate([front_half * cos_t - back_half * sin_t, front_half * sin_t + back_half * cos_t], axis=-1)


def reference(hidden, g_in, w_dq, g_q, w_dkv, g_kv, w_kr, w_uq, w_uk, w_uv, w_o):
    tokens = rms_norm(hidden, g_in).reshape(BATCH * SEQ, D)
    c_q = jnp.dot(tokens, w_dq, preferred_element_type=jnp.float32).astype(jnp.bfloat16)
    c_kv = jnp.dot(tokens, w_dkv, preferred_element_type=jnp.float32).astype(jnp.bfloat16)
    k_raw = jnp.dot(tokens, w_kr, preferred_element_type=jnp.float32).astype(jnp.bfloat16)
    cq_norm = rms_norm(c_q, g_q)
    ckv_norm = rms_norm(c_kv, g_kv)
    cos_t, sin_t = rope_tables()
    k_pe = rotate(k_raw.reshape(BATCH, SEQ, ROPE).astype(jnp.float32), cos_t, sin_t).astype(jnp.bfloat16)
    q_all = jnp.dot(cq_norm, w_uq.reshape(Q_LORA, HEADS * QK_DIM), preferred_element_type=jnp.float32)
    q_all = q_all.astype(jnp.bfloat16).reshape(BATCH, SEQ, HEADS, QK_DIM)
    q_nope = q_all[..., :NOPE]
    q_pe = rotate(q_all[..., NOPE:].astype(jnp.float32), cos_t[:, None, :], sin_t[:, None, :]).astype(jnp.bfloat16)
    k_nope = jnp.dot(ckv_norm, w_uk.reshape(KV_LORA, HEADS * NOPE), preferred_element_type=jnp.float32)
    k_nope = k_nope.astype(jnp.bfloat16).reshape(BATCH, SEQ, HEADS, NOPE)
    v_heads = jnp.dot(ckv_norm, w_uv.reshape(KV_LORA, HEADS * VDIM), preferred_element_type=jnp.float32)
    v_heads = v_heads.astype(jnp.bfloat16).reshape(BATCH, SEQ, HEADS, VDIM)
    key_pos = jnp.arange(SEQ)

    def attend_block(blk_idx):
        seq_idx = blk_idx // BLOCKS_PER_SEQ
        q_start = (blk_idx % BLOCKS_PER_SEQ) * Q_BLOCK
        qn_seq = lax.dynamic_index_in_dim(q_nope, seq_idx, 0, keepdims=False)
        qp_seq = lax.dynamic_index_in_dim(q_pe, seq_idx, 0, keepdims=False)
        qn_blk = lax.dynamic_slice_in_dim(qn_seq, q_start, Q_BLOCK, 0).astype(jnp.float32)
        qp_blk = lax.dynamic_slice_in_dim(qp_seq, q_start, Q_BLOCK, 0).astype(jnp.float32)
        kn_seq = lax.dynamic_index_in_dim(k_nope, seq_idx, 0, keepdims=False).astype(jnp.float32)
        kp_seq = lax.dynamic_index_in_dim(k_pe, seq_idx, 0, keepdims=False).astype(jnp.float32)
        v_seq = lax.dynamic_index_in_dim(v_heads, seq_idx, 0, keepdims=False).astype(jnp.float32)
        scores = jnp.einsum("qhd,khd->hqk", qn_blk, kn_seq) + jnp.einsum("qhr,kr->hqk", qp_blk, kp_seq)
        q_pos = q_start + jnp.arange(Q_BLOCK)
        allowed = key_pos[None, :] <= q_pos[:, None]
        scores = jnp.where(allowed[None, :, :], scores * SOFTMAX_SCALE, -jnp.inf)
        attn_prob = jax.nn.softmax(scores, axis=-1).astype(jnp.bfloat16).astype(jnp.float32)
        return jnp.einsum("hqk,khv->qhv", attn_prob, v_seq).astype(jnp.bfloat16)

    context = lax.map(attend_block, jnp.arange(NUM_BLOCKS)).reshape(BATCH * SEQ, HEADS * VDIM)
    attn_sum = jnp.dot(context, w_o.reshape(HEADS * VDIM, D), preferred_element_type=jnp.float32)
    result = (hidden.astype(jnp.float32) + attn_sum.reshape(BATCH, SEQ, D)).astype(jnp.bfloat16)
    return (result, ckv_norm.reshape(BATCH, SEQ, KV_LORA), k_pe)
```

```python
import functools
import math

import jax
import jax.numpy as jnp
from jax import lax
from jax.experimental import pallas as pl
from jax.experimental.pallas import tpu as pltpu
from jax.sharding import PartitionSpec as P

ROPE_BASE = 10000.0
NORM_EPS = 1.0e-6
MSCALE = 0.1 * math.log(40.0) + 1.0
LOG2E = math.log2(math.e)
F32 = jnp.float32
BF16 = jnp.bfloat16


def rope_rows(seq_len, rope_dim):
    half = rope_dim // 2
    inv_freq = ROPE_BASE ** (-2.0 * jnp.arange(half, dtype=F32) / rope_dim)
    angles = jnp.arange(seq_len, dtype=F32)[:, None] * inv_freq[None, :]
    c, s = jnp.cos(angles), jnp.sin(angles)
    return jnp.concatenate([c, c, c, c], -1), jnp.concatenate([-s, s, -s, s], -1)


def attn_kernel(heads, rope, cq_w, scale, lat_ref, own_ref, wq_ref, wk_ref, wv_ref, gown_ref, cos_ref, sin_ref, o_ref, small_ref):
    parts, width = lat_ref.shape[0], lat_ref.shape[3]
    seq = cos_ref.shape[0]
    nope = wk_ref.shape[1] // heads
    hd = nope + rope
    half = seq // 2
    pieces = [lat_ref[j, 0, :seq] for j in range(parts)]
    gains = [jnp.concatenate([lat_ref[j, 0, seq : seq + 1, width // 2 :], lat_ref[j, 0, seq + 1 : seq + 2, width // 2 :]], axis=-1).astype(F32) for j in range(parts)]
    gq = jnp.concatenate([g[:, :cq_w] for g in gains], axis=-1)
    gkv = jnp.concatenate([g[:, cq_w:] for g in gains], axis=-1)
    cq = jnp.concatenate([p[:, :cq_w] for p in pieces], axis=-1).astype(F32)
    ckv = jnp.concatenate([p[:, cq_w:] for p in pieces], axis=-1).astype(F32)
    rq = lax.rsqrt(jnp.mean(cq * cq, axis=-1, keepdims=True) + NORM_EPS)
    rkv = lax.rsqrt(jnp.mean(ckv * ckv, axis=-1, keepdims=True) + NORM_EPS)
    cqn = (cq * rq * gq).astype(BF16)
    ckvn = (ckv * rkv * gkv).astype(BF16)

    lane = lax.broadcasted_iota(jnp.int32, (seq, 2 * rope), 1)
    first = (lane % rope) < (rope // 2)
    cos_t, sin_t = cos_ref[...], sin_ref[...]

    def rot(x):
        swapped = jnp.where(first, pltpu.roll(x, 2 * rope - rope // 2, 1), pltpu.roll(x, rope // 2, 1))
        return (x * cos_t + swapped * sin_t).astype(BF16)

    own = own_ref[0, :seq].astype(F32)
    own_ckv = (own[:, cq_w:] * rkv * gown_ref[...].astype(F32)).astype(BF16)
    kpe2 = rot(jnp.concatenate([lat_ref[j, 0, seq:, : width // 2] for j in range(parts)], axis=0).astype(F32))
    small_ref[0] = jnp.concatenate([own_ckv, kpe2[:, :rope]], axis=-1)
    zero = jnp.zeros_like(kpe2)
    kpe = (jnp.where(lane < rope, kpe2, zero), jnp.where(lane >= rope, kpe2, zero))

    nt = (((1,), (1,)), ((), ()))

    def q_cols(first_col, count, ns):
        rows_t = jnp.concatenate([wq_ref[hd * n + first_col : hd * n + first_col + count, :] for n in ns], axis=0)
        return lax.dot_general(cqn, rows_t, nt, preferred_element_type=F32).astype(BF16)

    qn = [q_cols(0, nope, (n, n + 1)) for n in range(0, heads, 2)]
    qr = [q_cols(nope, rope, range(n, n + 4)).astype(F32) for n in range(0, heads, 4)]
    kn = jnp.dot(ckvn, wk_ref[...], preferred_element_type=F32).astype(BF16)
    vv = jnp.dot(ckvn, wv_ref[...], preferred_element_type=F32).astype(BF16)

    row = lax.broadcasted_iota(jnp.int32, (half, half), 0)
    col = lax.broadcasted_iota(jnp.int32, (half, half), 1)
    tri = col <= row
    c2 = scale * LOG2E
    for n in range(heads):
        if n % 2 == 0:
            qpe = rot(qr[n // 4][:, rope * (n % 4) : rope * (n % 4 + 2)])
        q = jnp.concatenate([qn[n // 2][:, nope * (n % 2) : nope * (n % 2 + 1)], qpe], axis=-1)
        k = jnp.concatenate([kn[:, nope * n : nope * (n + 1)], kpe[n % 2]], axis=-1)
        v = vv[:, nope * n : nope * (n + 1)]
        s0 = lax.dot_general(q[:half], k[:half], nt, preferred_element_type=F32)
        s1 = lax.dot_general(q[half:], k, nt, preferred_element_type=F32)
        s0 = jnp.where(tri, s0 * c2, -jnp.inf)
        e0 = jnp.exp2(s0 - jnp.max(s0, axis=-1, keepdims=True))
        p0 = (e0 / jnp.sum(e0, axis=-1, keepdims=True)).astype(BF16)
        sa = s1[:, :half] * c2
        sb = jnp.where(tri, s1[:, half:] * c2, -jnp.inf)
        m1 = jnp.max(jnp.maximum(sa, sb), axis=-1, keepdims=True)
        ea, eb = jnp.exp2(sa - m1), jnp.exp2(sb - m1)
        inv = 1.0 / jnp.sum(ea + eb, axis=-1, keepdims=True)
        p1 = jnp.concatenate([(ea * inv).astype(BF16), (eb * inv).astype(BF16)], axis=-1)
        o_ref[0, :half, nope * n : nope * (n + 1)] = jnp.dot(p0, v[:half], preferred_element_type=F32).astype(BF16)
        o_ref[0, half:, nope * n : nope * (n + 1)] = jnp.dot(p1, v, preferred_element_type=F32).astype(BF16)


def attention(lat, own, weights, gown, tables, scale, heads, rope, cq_w):
    parts, nseq, ext, width = lat.shape
    seq = tables[0].shape[0]
    whole = lambda a: pl.BlockSpec(a.shape, lambda s: (0,) * a.ndim)
    o_w = weights[2].shape[1]
    flops = 2 * nseq * seq * sum(w.shape[0] * w.shape[1] for w in weights) + 4 * nseq * heads * seq * seq * 256
    return pl.pallas_call(
        functools.partial(attn_kernel, heads, rope, cq_w, scale),
        grid=(nseq,),
        in_specs=[pl.BlockSpec((parts, 1, ext, width), lambda s: (0, s, 0, 0)), pl.BlockSpec((1, ext, width), lambda s: (s, 0, 0))] + [whole(a) for a in (*weights, gown, *tables)],
        out_specs=[pl.BlockSpec((1, seq, o_w), lambda s: (s, 0, 0)), pl.BlockSpec((1, seq, 2 * rope), lambda s: (s, 0, 0))],
        out_shape=[jax.ShapeDtypeStruct((nseq, seq, o_w), BF16), jax.ShapeDtypeStruct((nseq, seq, 2 * rope), BF16)],
        compiler_params=pltpu.CompilerParams(vmem_limit_bytes=60 * 1024 * 1024),
        cost_estimate=pl.CostEstimate(flops=flops, bytes_accessed=lat.size * 2, transcendentals=0),
        name="mla_attention",
    )(lat, own, *weights, gown, *tables)


MESH = pl.DeviceIdType.MESH


def tail_kernel(rows, o_hbm, w_ref, h_hbm, out_hbm, obuf, pall, precv, r2p, r2m, r1p, r1m, fin, hbuf, osend, orecv, hsend, hrecv, loc, s_snd, s_rcv, x_snd, x_rcv, g_snd, g_rcv, q_snd, q_rcv):
    y, j = lax.axis_index("emb"), lax.axis_index("head")
    emb, nown, seq, width = out_hbm.shape
    ring = nown // 2
    quarters = seq // rows
    units = emb * quarters
    hr = rows // 2
    x, c = j // 2, j % 2
    x_next, x_prev = (x + 1) % ring, (x + ring - 1) % ring
    x_far = (x + 2) % ring
    y_next, y_prev = (y + 1) % emb, (y + emb - 1) % emb
    to_next, to_prev = {"head": 2 * x_next + c}, {"head": 2 * x_prev + c}
    to_sib = {"head": 2 * x + 1 - c}
    to_up, to_down = {"emb": y_next}, {"emb": y_prev}
    half_k = nown // 2

    barrier = pltpu.get_barrier_semaphore()
    for dev in (to_next, to_prev, to_sib, to_up, to_down):
        pl.semaphore_signal(barrier, inc=1, device_id=dev, device_id_type=MESH)

    def remote(src, dst, ssem, rsem, dev):
        return pltpu.make_async_remote_copy(src_ref=src, dst_ref=dst, send_sem=ssem, recv_sem=rsem, device_id=dev, device_id_type=MESH)

    def own_in(r):
        return pltpu.make_async_copy(o_hbm.at[:, pl.ds(r * rows, rows), :], obuf.at[r], loc.at[r])

    h_in = pltpu.make_async_copy(h_hbm.at[:, j], hbuf, loc.at[quarters])
    for r in range(quarters):
        own_in(r).start()
    h_in.start()
    pl.semaphore_wait(barrier, 5)

    def o_down(r):
        return remote(obuf.at[r], obuf.at[quarters + 3 * r], osend.at[2 * r], orecv.at[2 * r], to_down)

    def o_up(r):
        return remote(obuf.at[r], obuf.at[quarters + 3 * r + 1], osend.at[2 * r + 1], orecv.at[2 * r + 1], to_up)

    def o_half_up(r):
        return remote(obuf.at[quarters + 3 * r + 1, pl.ds(0, half_k)], obuf.at[quarters + 3 * r + 2, pl.ds(0, half_k)], hsend.at[2 * r], hrecv.at[2 * r], to_up)

    def o_half_down(r):
        return remote(obuf.at[quarters + 3 * r, pl.ds(half_k, half_k)], obuf.at[quarters + 3 * r + 2, pl.ds(half_k, half_k)], hsend.at[2 * r + 1], hrecv.at[2 * r + 1], to_down)

    for r in range(quarters):
        own_in(r).wait()
        o_down(r).start()
        o_up(r).start()
    h_in.wait()

    def place(u):
        v = u - quarters
        w = v % 3
        off = 1 + 2 * w - 3 * (w // 2)
        is_own = u < quarters
        yy = jnp.where(is_own, y, (y + off) % emb)
        return yy, jnp.where(is_own, u, v // 3)

    def spot(ref, u, owner, lo, n):
        yy, r = place(u)
        return ref.at[yy, owner, pl.ds(r * rows + lo, n), :]

    def d2d(u):
        return remote(pall.at[u % 4, :, 1 - c], precv.at[u], s_snd.at[u], s_rcv.at[u], to_sib)

    def far_next(u):
        return remote(pall.at[u % 4, x_far, c, pl.ds(0, hr)], r2p.at[u], x_snd.at[0, u], x_rcv.at[0, u], to_next)

    def far_prev(u):
        return remote(pall.at[u % 4, x_far, c, pl.ds(hr, hr)], r2m.at[u], x_snd.at[1, u], x_rcv.at[1, u], to_prev)

    def near_next(u):
        return remote(pall.at[u % 4, x_next, c], r1p.at[u], x_snd.at[2, u], x_rcv.at[2, u], to_next)

    def near_prev(u):
        return remote(pall.at[u % 4, x_prev, c], r1m.at[u], x_snd.at[3, u], x_rcv.at[3, u], to_prev)

    def fin_local(u):
        return pltpu.make_async_copy(fin.at[u], spot(out_hbm, u, j, 0, rows), g_snd.at[3, u])

    def gather(u, owner, k, dev):
        return remote(fin.at[u], spot(out_hbm, u, owner, 0, rows), g_snd.at[k, u], g_rcv.at[k, u], dev)

    def relay(u, owner, lo, n, k, dev):
        return remote(spot(out_hbm, u, owner, lo, n), spot(out_hbm, u, owner, lo, n), q_snd.at[k, u], q_rcv.at[k, u], dev)

    own_next, own_prev, own_far = 2 * x_next + c, 2 * x_prev + c, 2 * x_far + c
    sib = 1 - 2 * c

    def stage_a(u):
        @pl.when(u >= quarters)
        def _():
            v = u - quarters
            r = v // 3

            @pl.when(v % 3 == 0)
            def _():
                o_down(r).wait_recv()
                o_half_down(r).start()

            @pl.when(v % 3 == 1)
            def _():
                o_up(r).wait_recv()
                o_half_up(r).start()

            @pl.when(v % 3 == 2)
            def _():
                o_half_up(r).wait_recv()
                o_half_down(r).wait_recv()

        @pl.when(u >= 4)
        def _():
            for cp in (d2d, far_next, far_prev, near_next, near_prev):
                cp(u - 4).wait_send()

        lhs = obuf[u].reshape(nown * rows, obuf.shape[3])
        tile = width // 3
        for n in range(3):
            res = jnp.dot(lhs, w_ref[:, n * tile : (n + 1) * tile], preferred_element_type=F32)
            pall[u % 4, :, :, :, n * tile : (n + 1) * tile] = res.astype(BF16).reshape(ring, 2, rows, tile)
        d2d(u).start()

    def stage_b(u):
        d2d(u).wait_recv()
        for i in range(ring):
            pall[u % 4, i, c] = (pall[u % 4, i, c].astype(F32) + precv[u, i].astype(F32)).astype(BF16)
        far_next(u).start()
        far_prev(u).start()

    def stage_c(u):
        far_next(u).wait_recv()
        pall[u % 4, x_next, c, pl.ds(0, hr)] = (pall[u % 4, x_next, c, pl.ds(0, hr)].astype(F32) + r2p[u].astype(F32)).astype(BF16)
        near_next(u).start()
        far_prev(u).wait_recv()
        pall[u % 4, x_prev, c, pl.ds(hr, hr)] = (pall[u % 4, x_prev, c, pl.ds(hr, hr)].astype(F32) + r2m[u].astype(F32)).astype(BF16)
        near_prev(u).start()

    def stage_d(u):
        near_next(u).wait_recv()
        near_prev(u).wait_recv()
        yy, r = place(u)
        total = pall[u % 4, x, c].astype(F32) + r1p[u].astype(F32) + r1m[u].astype(F32)
        fin[u] = (hbuf[yy, pl.ds(r * rows, rows)].astype(F32) + total).astype(BF16)
        gather(u, j, 0, to_next).start()
        gather(u, j, 1, to_prev).start()
        gather(u, j, 2, to_sib).start()
        fin_local(u).start()

    def stage_e(u):
        gather(u, own_prev, 0, to_next).wait_recv()
        relay(u, own_prev, 0, hr, 0, to_next).start()
        relay(u, own_prev, 0, rows, 2, to_sib).start()
        gather(u, own_next, 1, to_prev).wait_recv()
        relay(u, own_next, hr, hr, 1, to_prev).start()
        relay(u, own_next, 0, rows, 3, to_sib).start()

    def stage_g(u):
        relay(u, own_far, 0, hr, 0, to_next).wait_recv()
        relay(u, own_far, 0, hr, 4, to_sib).start()
        relay(u, own_far, hr, hr, 1, to_prev).wait_recv()
        relay(u, own_far, hr, hr, 5, to_sib).start()

    stages = (stage_a, stage_b, stage_c, stage_d, stage_e, stage_g)

    @pl.loop(0, units + len(stages) - 1)
    def _(t):
        for lag, stage in enumerate(stages):

            @pl.when((t >= lag) & (t < units + lag))
            def _():
                stage(t - lag)

    @pl.loop(0, units)
    def _(u):
        @pl.when(u >= units - 4)
        def _():
            for cp in (d2d, far_next, far_prev, near_next, near_prev):
                cp(u).wait_send()

        fin_local(u).wait()
        gather(u, j, 0, to_next).wait_send()
        gather(u, j, 1, to_prev).wait_send()
        gather(u, j, 2, to_sib).wait_send()
        relay(u, own_prev, 0, hr, 0, to_next).wait_send()
        relay(u, own_next, hr, hr, 1, to_prev).wait_send()
        relay(u, own_prev, 0, rows, 2, to_sib).wait_send()
        relay(u, own_next, 0, rows, 3, to_sib).wait_send()
        relay(u, own_far, 0, hr, 4, to_sib).wait_send()
        relay(u, own_far, hr, hr, 5, to_sib).wait_send()
        gather(u, j + sib, 2, to_sib).wait_recv()
        relay(u, own_prev + sib, 0, rows, 2, to_sib).wait_recv()
        relay(u, own_next + sib, 0, rows, 3, to_sib).wait_recv()
        relay(u, own_far + sib, 0, hr, 4, to_sib).wait_recv()
        relay(u, own_far + sib, hr, hr, 5, to_sib).wait_recv()

    for r in range(quarters):
        o_down(r).wait_send()
        o_up(r).wait_send()
        o_half_up(r).wait_send()
        o_half_down(r).wait_send()


def tail(o, w_o, hidden, emb):
    nseq, seq, depth = o.shape
    batch, _, width = hidden.shape
    assert batch == emb * nseq and emb == 4 and nseq == 8
    rows = seq // 4
    units = 4 * emb
    dma = pltpu.SemaphoreType.DMA
    h4 = hidden.reshape(emb, nseq, seq, width)
    out = pl.pallas_call(
        functools.partial(tail_kernel, rows),
        out_shape=jax.ShapeDtypeStruct(h4.shape, BF16),
        in_specs=[pl.BlockSpec(memory_space=pl.ANY), pl.BlockSpec(memory_space=pltpu.VMEM), pl.BlockSpec(memory_space=pl.ANY)],
        out_specs=pl.BlockSpec(memory_space=pl.ANY),
        scratch_shapes=[
            pltpu.VMEM((units, nseq, rows, depth), BF16),
            pltpu.VMEM((4, nseq // 2, 2, rows, width), BF16),
            pltpu.VMEM((units, nseq // 2, rows, width), BF16),
            pltpu.VMEM((units, rows // 2, width), BF16),
            pltpu.VMEM((units, rows // 2, width), BF16),
            pltpu.VMEM((units, rows, width), BF16),
            pltpu.VMEM((units, rows, width), BF16),
            pltpu.VMEM((units, rows, width), BF16),
            pltpu.VMEM((emb, seq, width), BF16),
            dma((8,)), dma((8,)), dma((8,)), dma((8,)), dma((5,)),
            dma((units,)), dma((units,)),
            dma((4, units)), dma((4, units)),
            dma((4, units)), dma((3, units)),
            dma((6, units)), dma((6, units)),
        ],
        compiler_params=pltpu.CompilerParams(collective_id=0, has_side_effects=True, vmem_limit_bytes=63 * 1024 * 1024),
        cost_estimate=pl.CostEstimate(flops=2 * batch * seq * depth * width, bytes_accessed=4 * batch * seq * width, transcendentals=0),
        name="mla_tail",
    )(o, w_o, h4)
    return out.reshape(batch, seq, width)


def latent_kernel(cq_w, ckv_w, kr_w, full_width, h_hbm, g_ref, w_ref, gains_ref, lat_hbm, own_hbm, hbuf, ssum, peers, pall, r2p, r2m, r1p, r1m, fin, h_sem, p_snd, p_rcv, y_snd, y_rcv, g_snd, g_rcv, q_snd, q_rcv):
    y, j = lax.axis_index("emb"), lax.axis_index("head")
    emb, nown, seq, width = h_hbm.shape
    units = nown
    ring = nown // 2
    ext = fin.shape[1]
    sub = seq // nown
    lat_w = cq_w + ckv_w
    hr = ext // 2
    x, c = j // 2, j % 2
    x_next, x_prev, x_far = (x + 1) % ring, (x + ring - 1) % ring, (x + 2) % ring
    y_next, y_prev, y_far = (y + 1) % emb, (y + emb - 1) % emb, (y + 2) % emb
    to_next, to_prev = {"head": 2 * x_next + c}, {"head": 2 * x_prev + c}
    to_sib = {"head": 2 * x + 1 - c}
    to_up, to_down, to_far = {"emb": y_next}, {"emb": y_prev}, {"emb": y_far}

    barrier = pltpu.get_barrier_semaphore()
    for dev in (to_next, to_prev, to_sib, to_up, to_down, to_far):
        pl.semaphore_signal(barrier, inc=1, device_id=dev, device_id_type=MESH)

    def remote(src, dst, ssem, rsem, dev):
        return pltpu.make_async_remote_copy(src_ref=src, dst_ref=dst, send_sem=ssem, recv_sem=rsem, device_id=dev, device_id_type=MESH)

    def h_in(s):
        return pltpu.make_async_copy(h_hbm.at[s // nown, s % nown], hbuf.at[s], h_sem.at[s])

    @pl.loop(0, emb * nown)
    def _(s):
        h_in(s).start()

    @pl.loop(0, emb * nown)
    def _(s):
        h_in(s).wait()
        acc = jnp.zeros((seq, 128), F32)
        for n in range(width // 128):
            piece = hbuf[s, :, 128 * n : 128 * (n + 1)].astype(F32)
            acc += piece * piece
        ssum[s // 8, pl.ds(s % 8, 1), :] = jnp.sum(acc.T, axis=0, keepdims=True)

    pl.semaphore_wait(barrier, 6)

    def stat(k, dev):
        return remote(ssum, peers.at[k], p_snd.at[k], p_rcv.at[k], dev)

    stats = (stat(0, to_up), stat(1, to_down), stat(2, to_far))
    for cp in stats:
        cp.start()
    for cp in stats:
        cp.wait_recv()

    def far_up(u):
        return remote(pall.at[u, y_far, pl.ds(0, hr)], r2p.at[u], y_snd.at[0, u], y_rcv.at[0, u], to_up)

    def far_down(u):
        return remote(pall.at[u, y_far, pl.ds(hr, hr)], r2m.at[u], y_snd.at[1, u], y_rcv.at[1, u], to_down)

    def near_up(u):
        return remote(pall.at[u, y_next], r1p.at[u], y_snd.at[2, u], y_rcv.at[2, u], to_up)

    def near_down(u):
        return remote(pall.at[u, y_prev], r1m.at[u], y_snd.at[3, u], y_rcv.at[3, u], to_down)

    def local(u, k):
        return pltpu.make_async_copy(fin.at[u], own_hbm.at[u] if k else lat_hbm.at[j, u], g_snd.at[3 + k, u])

    def gather(u, owner, k, dev):
        return remote(fin.at[u], lat_hbm.at[owner, u], g_snd.at[k, u], g_rcv.at[k, u], dev)

    def relay(u, owner, lo, n, k, dev):
        part = lat_hbm.at[owner, u, pl.ds(lo, n), :]
        return remote(part, part, q_snd.at[k, u], q_rcv.at[k, u], dev)

    own_next, own_prev, own_far = 2 * x_next + c, 2 * x_prev + c, 2 * x_far + c
    sib = 1 - 2 * c
    nt = (((1,), (1,)), ((), ()))

    def stage_a(u):
        @pl.loop(0, emb)
        def _(yy):
            s = yy * nown + u
            ss = ssum[s // 8, pl.ds(s % 8, 1), :]
            for k in range(3):
                ss = ss + peers[k, s // 8, pl.ds(s % 8, 1), :]
            r_row = lax.rsqrt(ss / full_width + NORM_EPS)
            r = jnp.broadcast_to(r_row, (128, seq)).T
            hn = []
            for n in range(width // 128):
                piece = hbuf[s, :, 128 * n : 128 * (n + 1)].astype(F32)
                hn.append((piece * r * g_ref[:, 128 * n : 128 * (n + 1)].astype(F32)).astype(BF16))
            hn = jnp.concatenate(hn, axis=-1)
            hbuf[s] = hn
            pall[u, yy, pl.ds(0, seq), :] = lax.dot_general(hn, w_ref[pl.ds(0, lat_w), :], nt, preferred_element_type=F32).astype(BF16)
            mine = hbuf[s, pl.ds(j * sub, sub), :]
            kr = lax.dot_general(mine, w_ref[pl.ds(lat_w, 2 * kr_w), :], nt, preferred_element_type=F32).astype(BF16)
            pall[u, yy, pl.ds(seq, sub), pl.ds(0, 2 * kr_w)] = kr
            pall[u, yy, pl.ds(seq, sub), pl.ds(2 * kr_w, 2 * kr_w)] = jnp.zeros_like(kr)

        far_up(u).start()
        far_down(u).start()

    def stage_b(u):
        far_up(u).wait_recv()
        pall[u, y_next, pl.ds(0, hr)] = (pall[u, y_next, pl.ds(0, hr)].astype(F32) + r2p[u].astype(F32)).astype(BF16)
        near_up(u).start()
        far_down(u).wait_recv()
        pall[u, y_prev, pl.ds(hr, hr)] = (pall[u, y_prev, pl.ds(hr, hr)].astype(F32) + r2m[u].astype(F32)).astype(BF16)
        near_down(u).start()

    def stage_c(u):
        near_up(u).wait_recv()
        near_down(u).wait_recv()
        fin[u] = (pall[u, y].astype(F32) + r1p[u].astype(F32) + r1m[u].astype(F32)).astype(BF16)
        fin[u, pl.ds(seq, sub), pl.ds(2 * kr_w, 2 * kr_w)] = gains_ref[...]
        gather(u, j, 0, to_next).start()
        gather(u, j, 1, to_prev).start()
        gather(u, j, 2, to_sib).start()
        local(u, 0).start()
        local(u, 1).start()

    def stage_d(u):
        gather(u, own_prev, 0, to_next).wait_recv()
        relay(u, own_prev, 0, hr, 0, to_next).start()
        relay(u, own_prev, 0, ext, 2, to_sib).start()
        gather(u, own_next, 1, to_prev).wait_recv()
        relay(u, own_next, hr, hr, 1, to_prev).start()
        relay(u, own_next, 0, ext, 3, to_sib).start()

    def stage_e(u):
        relay(u, own_far, 0, hr, 0, to_next).wait_recv()
        relay(u, own_far, 0, hr, 4, to_sib).start()
        relay(u, own_far, hr, hr, 1, to_prev).wait_recv()
        relay(u, own_far, hr, hr, 5, to_sib).start()

    stages = (stage_a, stage_b, stage_c, stage_d, stage_e)

    @pl.loop(0, units + len(stages) - 1)
    def _(t):
        for lag, stage in enumerate(stages):

            @pl.when((t >= lag) & (t < units + lag))
            def _():
                stage(t - lag)

    @pl.loop(0, units)
    def _(u):
        for cp in (far_up, far_down, near_up, near_down):
            cp(u).wait_send()
        local(u, 0).wait()
        local(u, 1).wait()
        gather(u, j, 0, to_next).wait_send()
        gather(u, j, 1, to_prev).wait_send()
        gather(u, j, 2, to_sib).wait_send()
        relay(u, own_prev, 0, hr, 0, to_next).wait_send()
        relay(u, own_next, hr, hr, 1, to_prev).wait_send()
        relay(u, own_prev, 0, ext, 2, to_sib).wait_send()
        relay(u, own_next, 0, ext, 3, to_sib).wait_send()
        relay(u, own_far, 0, hr, 4, to_sib).wait_send()
        relay(u, own_far, hr, hr, 5, to_sib).wait_send()
        gather(u, j + sib, 2, to_sib).wait_recv()
        relay(u, own_prev + sib, 0, ext, 2, to_sib).wait_recv()
        relay(u, own_next + sib, 0, ext, 3, to_sib).wait_recv()
        relay(u, own_far + sib, 0, hr, 4, to_sib).wait_recv()
        relay(u, own_far + sib, hr, hr, 5, to_sib).wait_recv()

    for cp in stats:
        cp.wait_send()


def latents(h4, g_in, w_t, gains, cq_w, ckv_w, kr_w):
    emb, nseq, seq, width = h4.shape
    lat_w = cq_w + ckv_w
    assert emb == 4 and nseq == 8 and lat_w == 4 * kr_w
    ext = seq + seq // nseq
    dma = pltpu.SemaphoreType.DMA
    vm = pl.BlockSpec(memory_space=pltpu.VMEM)
    hbm = pl.BlockSpec(memory_space=pl.ANY)
    return pl.pallas_call(
        functools.partial(latent_kernel, cq_w, ckv_w, kr_w, width * emb),
        out_shape=[jax.ShapeDtypeStruct((nseq, nseq, ext, lat_w), BF16), jax.ShapeDtypeStruct((nseq, ext, lat_w), BF16)],
        in_specs=[hbm, vm, vm, vm],
        out_specs=[hbm, hbm],
        scratch_shapes=[
            pltpu.VMEM((emb * nseq, seq, width), BF16),
            pltpu.VMEM((emb * nseq // 8, 8, seq), F32),
            pltpu.VMEM((3, emb * nseq // 8, 8, seq), F32),
            pltpu.VMEM((nseq, emb, ext, lat_w), BF16),
            pltpu.VMEM((nseq, ext // 2, lat_w), BF16),
            pltpu.VMEM((nseq, ext // 2, lat_w), BF16),
            pltpu.VMEM((nseq, ext, lat_w), BF16),
            pltpu.VMEM((nseq, ext, lat_w), BF16),
            pltpu.VMEM((nseq, ext, lat_w), BF16),
            dma((emb * nseq,)), dma((3,)), dma((3,)),
            dma((4, nseq)), dma((4, nseq)),
            dma((5, nseq)), dma((3, nseq)),
            dma((6, nseq)), dma((6, nseq)),
        ],
        compiler_params=pltpu.CompilerParams(collective_id=1, has_side_effects=True, vmem_limit_bytes=60 * 1024 * 1024),
        cost_estimate=pl.CostEstimate(flops=2 * emb * nseq * seq * width * lat_w, bytes_accessed=2 * emb * nseq * seq * width, transcendentals=0),
        name="mla_latents",
    )(h4, g_in, w_t, gains)


def solution(mesh):
    emb_count = mesh.shape["emb"]
    in_specs = (P("dp", None, "emb"), P("emb"), P("emb", "head"), P("head"), P("emb", "head"), P("head"), P("emb", None), P(None, "head", None), P(None, "head", None), P(None, "head", None), P("head", None, "emb"))
    out_specs = (P("dp", None, "emb"), P("dp", None, "head"), P("dp", None, None))

    def local_block(hidden, g_in, w_dq, g_q, w_dkv, g_kv, w_kr, w_uq, w_uk, w_uv, w_o):
        batch, seq, width = hidden.shape
        nope, rope = w_uk.shape[2], w_kr.shape[1]
        heads = w_uq.shape[1]
        cq_w, ckv_w = w_dq.shape[1], w_dkv.shape[1]
        scale = MSCALE * MSCALE / math.sqrt(w_uq.shape[2])
        w_t = jnp.concatenate([w_dq.T, w_dkv.T, w_kr.T, w_kr.T], axis=0)
        g_loc = jnp.concatenate([g_q, g_kv]).reshape(2, 2 * rope)
        gains = jnp.pad(g_loc, ((0, seq // (batch // emb_count) - 2), (0, 0)))
        h4 = hidden.reshape(emb_count, batch // emb_count, seq, width)
        lat, own = latents(h4, g_in[None], w_t, gains, cq_w, ckv_w, rope)
        weights = (
            w_uq.transpose(1, 2, 0).reshape(-1, w_uq.shape[0]),
            w_uk.reshape(w_uk.shape[0], heads * nope),
            w_uv.reshape(w_uv.shape[0], -1),
        )
        o, small = attention(lat, own, weights, g_kv[None], rope_rows(seq, rope), scale, heads, rope, cq_w)
        small_all = lax.all_gather(small, "emb", axis=0, tiled=True)
        result = tail(o, w_o.reshape(-1, w_o.shape[2]), hidden, emb_count)
        return result, small_all[..., :ckv_w], small_all[..., ckv_w:]

    return jax.shard_map(local_block, mesh=mesh, in_specs=in_specs, out_specs=out_specs, check_vma=False)
```

```python
import functools
import math

import jax
import jax.numpy as jnp
from jax import lax
from jax.experimental import pallas as pl
from jax.experimental.pallas import tpu as pltpu
from jax.sharding import PartitionSpec as P

ROPE_BASE = 10000.0
NORM_EPS = 1.0e-6
MSCALE = 0.1 * math.log(40.0) + 1.0
LOG2E = math.log2(math.e)
F32 = jnp.float32
BF16 = jnp.bfloat16


def rope_rows(seq_len, rope_dim):
    half = rope_dim // 2
    inv_freq = ROPE_BASE ** (-2.0 * jnp.arange(half, dtype=F32) / rope_dim)
    angles = jnp.arange(seq_len, dtype=F32)[:, None] * inv_freq[None, :]
    c, s = jnp.cos(angles), jnp.sin(angles)
    return jnp.concatenate([c, c, c, c], -1), jnp.concatenate([-s, s, -s, s], -1)


def attn_kernel(heads, rope, cq_w, scale, lat_ref, own_ref, wq_ref, wk_ref, wv_ref, gown_ref, cos_ref, sin_ref, o_ref, small_ref):
    parts, width = lat_ref.shape[0], lat_ref.shape[3]
    seq = cos_ref.shape[0]
    nope = wk_ref.shape[1] // heads
    hd = nope + rope
    half = seq // 2
    pieces = [lat_ref[j, 0, :seq] for j in range(parts)]
    gains = [jnp.concatenate([lat_ref[j, 0, seq : seq + 1, width // 2 :], lat_ref[j, 0, seq + 1 : seq + 2, width // 2 :]], axis=-1).astype(F32) for j in range(parts)]
    gq = jnp.concatenate([g[:, :cq_w] for g in gains], axis=-1)
    gkv = jnp.concatenate([g[:, cq_w:] for g in gains], axis=-1)
    cq = jnp.concatenate([p[:, :cq_w] for p in pieces], axis=-1).astype(F32)
    ckv = jnp.concatenate([p[:, cq_w:] for p in pieces], axis=-1).astype(F32)
    rq = lax.rsqrt(jnp.mean(cq * cq, axis=-1, keepdims=True) + NORM_EPS)
    rkv = lax.rsqrt(jnp.mean(ckv * ckv, axis=-1, keepdims=True) + NORM_EPS)
    cqn = (cq * rq * gq).astype(BF16)
    ckvn = (ckv * rkv * gkv).astype(BF16)

    lane = lax.broadcasted_iota(jnp.int32, (seq, 2 * rope), 1)
    first = (lane % rope) < (rope // 2)
    cos_t, sin_t = cos_ref[...], sin_ref[...]

    def rot(x):
        swapped = jnp.where(first, pltpu.roll(x, 2 * rope - rope // 2, 1), pltpu.roll(x, rope // 2, 1))
        return (x * cos_t + swapped * sin_t).astype(BF16)

    own = own_ref[0, :seq].astype(F32)
    own_ckv = (own[:, cq_w:] * rkv * gown_ref[...].astype(F32)).astype(BF16)
    kpe2 = rot(jnp.concatenate([lat_ref[j, 0, seq:, : width // 2] for j in range(parts)], axis=0).astype(F32))
    small_ref[0] = jnp.concatenate([own_ckv, kpe2[:, :rope]], axis=-1).astype(F32).T.astype(BF16)
    zero = jnp.zeros_like(kpe2)
    kpe = (jnp.where(lane < rope, kpe2, zero), jnp.where(lane >= rope, kpe2, zero))

    nt = (((1,), (1,)), ((), ()))

    def q_cols(first_col, count, ns):
        rows_t = jnp.concatenate([wq_ref[hd * n + first_col : hd * n + first_col + count, :] for n in ns], axis=0)
        return lax.dot_general(cqn, rows_t, nt, preferred_element_type=F32).astype(BF16)

    qn = [q_cols(0, nope, (n, n + 1)) for n in range(0, heads, 2)]
    qr = [q_cols(nope, rope, range(n, n + 4)).astype(F32) for n in range(0, heads, 4)]
    kn = jnp.dot(ckvn, wk_ref[...], preferred_element_type=F32).astype(BF16)
    vv = jnp.dot(ckvn, wv_ref[...], preferred_element_type=F32).astype(BF16)

    row = lax.broadcasted_iota(jnp.int32, (half, half), 0)
    col = lax.broadcasted_iota(jnp.int32, (half, half), 1)
    tri = col <= row
    c2 = scale * LOG2E
    for n in range(heads):
        if n % 2 == 0:
            qpe = rot(qr[n // 4][:, rope * (n % 4) : rope * (n % 4 + 2)])
        q = jnp.concatenate([qn[n // 2][:, nope * (n % 2) : nope * (n % 2 + 1)], qpe], axis=-1)
        k = jnp.concatenate([kn[:, nope * n : nope * (n + 1)], kpe[n % 2]], axis=-1)
        v = vv[:, nope * n : nope * (n + 1)]
        s0 = lax.dot_general(q[:half], k[:half], nt, preferred_element_type=F32)
        s1 = lax.dot_general(q[half:], k, nt, preferred_element_type=F32)
        s0 = jnp.where(tri, s0 * c2, -jnp.inf)
        e0 = jnp.exp2(s0 - jnp.max(s0, axis=-1, keepdims=True))
        p0 = (e0 / jnp.sum(e0, axis=-1, keepdims=True)).astype(BF16)
        sa = s1[:, :half] * c2
        sb = jnp.where(tri, s1[:, half:] * c2, -jnp.inf)
        m1 = jnp.max(jnp.maximum(sa, sb), axis=-1, keepdims=True)
        ea, eb = jnp.exp2(sa - m1), jnp.exp2(sb - m1)
        inv = 1.0 / jnp.sum(ea + eb, axis=-1, keepdims=True)
        p1 = jnp.concatenate([(ea * inv).astype(BF16), (eb * inv).astype(BF16)], axis=-1)
        o_ref[0, :half, nope * n : nope * (n + 1)] = jnp.dot(p0, v[:half], preferred_element_type=F32).astype(BF16)
        o_ref[0, half:, nope * n : nope * (n + 1)] = jnp.dot(p1, v, preferred_element_type=F32).astype(BF16)


def attention(lat, own, weights, gown, tables, scale, heads, rope, cq_w):
    parts, nseq, ext, width = lat.shape
    seq = tables[0].shape[0]
    whole = lambda a: pl.BlockSpec(a.shape, lambda s: (0,) * a.ndim)
    o_w = weights[2].shape[1]
    flops = 2 * nseq * seq * sum(w.shape[0] * w.shape[1] for w in weights) + 4 * nseq * heads * seq * seq * 256
    return pl.pallas_call(
        functools.partial(attn_kernel, heads, rope, cq_w, scale),
        grid=(nseq,),
        in_specs=[pl.BlockSpec((parts, 1, ext, width), lambda s: (0, s, 0, 0)), pl.BlockSpec((1, ext, width), lambda s: (s, 0, 0))] + [whole(a) for a in (*weights, gown, *tables)],
        out_specs=[pl.BlockSpec((1, seq, o_w), lambda s: (s, 0, 0)), pl.BlockSpec((1, 2 * rope, seq), lambda s: (s, 0, 0))],
        out_shape=[jax.ShapeDtypeStruct((nseq, seq, o_w), BF16), jax.ShapeDtypeStruct((nseq, 2 * rope, seq), BF16)],
        compiler_params=pltpu.CompilerParams(vmem_limit_bytes=60 * 1024 * 1024),
        cost_estimate=pl.CostEstimate(flops=flops, bytes_accessed=lat.size * 2, transcendentals=0),
        name="mla_attention",
    )(lat, own, *weights, gown, *tables)


MESH = pl.DeviceIdType.MESH


def tail_kernel(rows, o_hbm, w_ref, h_hbm, sm_hbm, out_hbm, smo_hbm, sbuf, sm_loc, sm_snd, sm_rcv, obuf, pall, precv, r2p, r2m, r1p, r1m, fin, hbuf, osend, orecv, hsend, hrecv, loc, s_snd, s_rcv, x_snd, x_rcv, g_snd, g_rcv, q_snd, q_rcv):
    y, j = lax.axis_index("emb"), lax.axis_index("head")
    emb, nown, seq, width = out_hbm.shape
    ring = nown // 2
    quarters = seq // rows
    units = emb * quarters
    hr = rows // 2
    x, c = j // 2, j % 2
    x_next, x_prev = (x + 1) % ring, (x + ring - 1) % ring
    x_far = (x + 2) % ring
    y_next, y_prev = (y + 1) % emb, (y + emb - 1) % emb
    to_next, to_prev = {"head": 2 * x_next + c}, {"head": 2 * x_prev + c}
    to_sib = {"head": 2 * x + 1 - c}
    to_up, to_down, to_opp = {"emb": y_next}, {"emb": y_prev}, {"emb": (y + 2) % emb}
    lead = quarters // 2
    half_k = nown // 2

    barrier = pltpu.get_barrier_semaphore()
    for dev in (to_next, to_prev, to_sib, to_up, to_down, to_opp):
        pl.semaphore_signal(barrier, inc=1, device_id=dev, device_id_type=MESH)

    def remote(src, dst, ssem, rsem, dev):
        return pltpu.make_async_remote_copy(src_ref=src, dst_ref=dst, send_sem=ssem, recv_sem=rsem, device_id=dev, device_id_type=MESH)

    def own_in(r):
        return pltpu.make_async_copy(o_hbm.at[:, pl.ds(r * rows, rows), :], obuf.at[r], loc.at[r])

    h_in = pltpu.make_async_copy(h_hbm.at[:, j], hbuf, loc.at[quarters])
    for r in range(quarters):
        own_in(r).start()
    sm_in = pltpu.make_async_copy(sm_hbm, sbuf, sm_loc.at[0])
    sm_own = pltpu.make_async_copy(sbuf, smo_hbm.at[y], sm_loc.at[1])
    h_in.start()
    sm_in.start()
    pl.semaphore_wait(barrier, 6)

    def sm_copy(k, dev):
        return remote(sbuf, smo_hbm.at[y], sm_snd.at[k], sm_rcv.at[k], dev)

    sm_copies = (sm_copy(0, to_up), sm_copy(1, to_down), sm_copy(2, to_opp))

    def o_down(r):
        return remote(obuf.at[r], obuf.at[quarters + 3 * r], osend.at[2 * r], orecv.at[2 * r], to_down)

    def o_up(r):
        return remote(obuf.at[r], obuf.at[quarters + 3 * r + 1], osend.at[2 * r + 1], orecv.at[2 * r + 1], to_up)

    def o_half_up(r):
        return remote(obuf.at[quarters + 3 * r + 1, pl.ds(0, half_k)], obuf.at[quarters + 3 * r + 2, pl.ds(0, half_k)], hsend.at[2 * r], hrecv.at[2 * r], to_up)

    def o_half_down(r):
        return remote(obuf.at[quarters + 3 * r, pl.ds(half_k, half_k)], obuf.at[quarters + 3 * r + 2, pl.ds(half_k, half_k)], hsend.at[2 * r + 1], hrecv.at[2 * r + 1], to_down)

    for r in range(quarters):
        own_in(r).wait()
        if r < lead:
            o_down(r).start()
            o_up(r).start()
    h_in.wait()
    sm_in.wait()
    sm_own.start()

    def place(u):
        v = u - quarters
        w = v % 3
        off = 1 + 2 * w - 3 * (w // 2)
        is_own = u < quarters
        yy = jnp.where(is_own, y, (y + off) % emb)
        return yy, jnp.where(is_own, u, v // 3)

    def spot(ref, u, owner, lo, n):
        yy, r = place(u)
        return ref.at[yy, owner, pl.ds(r * rows + lo, n), :]

    def d2d(u):
        return remote(pall.at[u % 4, :, 1 - c], precv.at[u], s_snd.at[u], s_rcv.at[u], to_sib)

    def far_next(u):
        return remote(pall.at[u % 4, x_far, c, pl.ds(0, hr)], r2p.at[u], x_snd.at[0, u], x_rcv.at[0, u], to_next)

    def far_prev(u):
        return remote(pall.at[u % 4, x_far, c, pl.ds(hr, hr)], r2m.at[u], x_snd.at[1, u], x_rcv.at[1, u], to_prev)

    def near_next(u):
        return remote(pall.at[u % 4, x_next, c], r1p.at[u], x_snd.at[2, u], x_rcv.at[2, u], to_next)

    def near_prev(u):
        return remote(pall.at[u % 4, x_prev, c], r1m.at[u], x_snd.at[3, u], x_rcv.at[3, u], to_prev)

    def fin_local(u):
        return pltpu.make_async_copy(fin.at[u], spot(out_hbm, u, j, 0, rows), g_snd.at[3, u])

    def gather(u, owner, k, dev):
        return remote(fin.at[u], spot(out_hbm, u, owner, 0, rows), g_snd.at[k, u], g_rcv.at[k, u], dev)

    def relay(u, owner, lo, n, k, dev):
        return remote(spot(out_hbm, u, owner, lo, n), spot(out_hbm, u, owner, lo, n), q_snd.at[k, u], q_rcv.at[k, u], dev)

    own_next, own_prev, own_far = 2 * x_next + c, 2 * x_prev + c, 2 * x_far + c
    sib = 1 - 2 * c

    def stage_a(u):
        @pl.when(u >= quarters)
        def _():
            v = u - quarters
            r = v // 3

            @pl.when(v % 3 == 2)
            def _():
                o_half_up(r).wait_recv()
                o_half_down(r).wait_recv()

        @pl.when(u >= 4)
        def _():
            for cp in (d2d, far_next, far_prev, near_next, near_prev):
                cp(u - 4).wait_send()

        lhs = obuf[u].reshape(nown * rows, obuf.shape[3])
        tile = width // 3
        for n in range(3):
            res = jnp.dot(lhs, w_ref[:, n * tile : (n + 1) * tile], preferred_element_type=F32)
            pall[u % 4, :, :, :, n * tile : (n + 1) * tile] = res.astype(BF16).reshape(ring, 2, rows, tile)
        d2d(u).start()

    def stage_b(u):
        d2d(u).wait_recv()
        for i in range(ring):
            pall[u % 4, i, c] = (pall[u % 4, i, c].astype(F32) + precv[u, i].astype(F32)).astype(BF16)
        far_next(u).start()
        far_prev(u).start()

    def stage_c(u):
        far_next(u).wait_recv()
        pall[u % 4, x_next, c, pl.ds(0, hr)] = (pall[u % 4, x_next, c, pl.ds(0, hr)].astype(F32) + r2p[u].astype(F32)).astype(BF16)
        near_next(u).start()
        far_prev(u).wait_recv()
        pall[u % 4, x_prev, c, pl.ds(hr, hr)] = (pall[u % 4, x_prev, c, pl.ds(hr, hr)].astype(F32) + r2m[u].astype(F32)).astype(BF16)
        near_prev(u).start()

    def stage_d(u):
        near_next(u).wait_recv()
        near_prev(u).wait_recv()
        yy, r = place(u)
        total = pall[u % 4, x, c].astype(F32) + r1p[u].astype(F32) + r1m[u].astype(F32)
        fin[u] = (hbuf[yy, pl.ds(r * rows, rows)].astype(F32) + total).astype(BF16)
        gather(u, j, 0, to_next).start()
        gather(u, j, 1, to_prev).start()
        gather(u, j, 2, to_sib).start()
        fin_local(u).start()

    def stage_e(u):
        gather(u, own_prev, 0, to_next).wait_recv()
        relay(u, own_prev, 0, hr, 0, to_next).start()
        relay(u, own_prev, 0, rows, 2, to_sib).start()
        gather(u, own_next, 1, to_prev).wait_recv()
        relay(u, own_next, hr, hr, 1, to_prev).start()
        relay(u, own_next, 0, rows, 3, to_sib).start()

    def stage_g(u):
        relay(u, own_far, 0, hr, 0, to_next).wait_recv()
        relay(u, own_far, 0, hr, 4, to_sib).start()
        relay(u, own_far, hr, hr, 1, to_prev).wait_recv()
        relay(u, own_far, hr, hr, 5, to_sib).start()

    stages = (stage_a, stage_b, stage_c, stage_d, stage_e, stage_g)

    @pl.loop(0, units + len(stages) - 1)
    def _(t):
        for lag, stage in enumerate(stages):

            @pl.when((t >= lag) & (t < units + lag))
            def _():
                stage(t - lag)

        ahead = t - (quarters - 1)

        @pl.when((ahead >= 0) & (ahead % 3 == 0) & (ahead < 3 * quarters))
        def _():
            r = ahead // 3
            o_down(r).wait_recv()
            o_half_down(r).start()
            o_up(r).wait_recv()
            o_half_up(r).start()

            @pl.when(r + lead < quarters)
            def _():
                o_down(r + lead).start()
                o_up(r + lead).start()

            @pl.when(r == quarters - 1)
            def _():
                for cp in sm_copies:
                    cp.start()

    for k, src in enumerate((y_prev, y_next, (y + 2) % emb)):
        remote(sbuf, smo_hbm.at[src], sm_snd.at[k], sm_rcv.at[k], to_up).wait_recv()
    for cp in sm_copies:
        cp.wait_send()
    sm_own.wait()

    @pl.loop(0, units)
    def _(u):
        @pl.when(u >= units - 4)
        def _():
            for cp in (d2d, far_next, far_prev, near_next, near_prev):
                cp(u).wait_send()

        fin_local(u).wait()
        gather(u, j, 0, to_next).wait_send()
        gather(u, j, 1, to_prev).wait_send()
        gather(u, j, 2, to_sib).wait_send()
        relay(u, own_prev, 0, hr, 0, to_next).wait_send()
        relay(u, own_next, hr, hr, 1, to_prev).wait_send()
        relay(u, own_prev, 0, rows, 2, to_sib).wait_send()
        relay(u, own_next, 0, rows, 3, to_sib).wait_send()
        relay(u, own_far, 0, hr, 4, to_sib).wait_send()
        relay(u, own_far, hr, hr, 5, to_sib).wait_send()
        gather(u, j + sib, 2, to_sib).wait_recv()
        relay(u, own_prev + sib, 0, rows, 2, to_sib).wait_recv()
        relay(u, own_next + sib, 0, rows, 3, to_sib).wait_recv()
        relay(u, own_far + sib, 0, hr, 4, to_sib).wait_recv()
        relay(u, own_far + sib, hr, hr, 5, to_sib).wait_recv()

    for r in range(quarters):
        o_down(r).wait_send()
        o_up(r).wait_send()
        o_half_up(r).wait_send()
        o_half_down(r).wait_send()


def tail(o, w_o, hidden, small, emb):
    nseq, seq, depth = o.shape
    batch, _, width = hidden.shape
    assert batch == emb * nseq and emb == 4 and nseq == 8
    parts = 4
    rows = seq // parts
    units = parts * emb
    dma = pltpu.SemaphoreType.DMA
    h4 = hidden.reshape(emb, nseq, seq, width)
    out, small_all = pl.pallas_call(
        functools.partial(tail_kernel, rows),
        out_shape=[jax.ShapeDtypeStruct(h4.shape, BF16), jax.ShapeDtypeStruct((emb,) + small.shape, BF16)],
        in_specs=[pl.BlockSpec(memory_space=pl.ANY), pl.BlockSpec(memory_space=pltpu.VMEM), pl.BlockSpec(memory_space=pl.ANY), pl.BlockSpec(memory_space=pl.ANY)],
        out_specs=[pl.BlockSpec(memory_space=pl.ANY), pl.BlockSpec(memory_space=pl.ANY)],
        scratch_shapes=[
            pltpu.VMEM(small.shape, BF16), dma((2,)), dma((3,)), dma((3,)),
            pltpu.VMEM((units, nseq, rows, depth), BF16),
            pltpu.VMEM((4, nseq // 2, 2, rows, width), BF16),
            pltpu.VMEM((units, nseq // 2, rows, width), BF16),
            pltpu.VMEM((units, rows // 2, width), BF16),
            pltpu.VMEM((units, rows // 2, width), BF16),
            pltpu.VMEM((units, rows, width), BF16),
            pltpu.VMEM((units, rows, width), BF16),
            pltpu.VMEM((units, rows, width), BF16),
            pltpu.VMEM((emb, seq, width), BF16),
            dma((2 * parts,)), dma((2 * parts,)), dma((2 * parts,)), dma((2 * parts,)), dma((parts + 1,)),
            dma((units,)), dma((units,)),
            dma((4, units)), dma((4, units)),
            dma((4, units)), dma((3, units)),
            dma((6, units)), dma((6, units)),
        ],
        compiler_params=pltpu.CompilerParams(collective_id=0, has_side_effects=True, vmem_limit_bytes=63 * 1024 * 1024),
        cost_estimate=pl.CostEstimate(flops=2 * batch * seq * depth * width, bytes_accessed=4 * batch * seq * width, transcendentals=0),
        name="mla_tail",
    )(o, w_o, h4, small)
    return out.reshape(batch, seq, width), small_all.reshape(batch, small.shape[1], seq)


def latent_kernel(cq_w, ckv_w, kr_w, full_width, h_hbm, g_ref, w_ref, gains_ref, lat_hbm, own_hbm, hbuf, ssum, peers, pall, r2p, r2m, r1p, r1m, fin, h_sem, p_snd, p_rcv, y_snd, y_rcv, g_snd, g_rcv, q_snd, q_rcv):
    y, j = lax.axis_index("emb"), lax.axis_index("head")
    emb, nown, seq, width = h_hbm.shape
    units = nown
    ring = nown // 2
    ext = fin.shape[1]
    sub = seq // nown
    lat_w = cq_w + ckv_w
    hr = ext // 2
    x, c = j // 2, j % 2
    x_next, x_prev, x_far = (x + 1) % ring, (x + ring - 1) % ring, (x + 2) % ring
    y_next, y_prev, y_far = (y + 1) % emb, (y + emb - 1) % emb, (y + 2) % emb
    to_next, to_prev = {"head": 2 * x_next + c}, {"head": 2 * x_prev + c}
    to_sib = {"head": 2 * x + 1 - c}
    to_up, to_down, to_far = {"emb": y_next}, {"emb": y_prev}, {"emb": y_far}

    barrier = pltpu.get_barrier_semaphore()
    for dev in (to_next, to_prev, to_sib, to_up, to_down, to_far):
        pl.semaphore_signal(barrier, inc=1, device_id=dev, device_id_type=MESH)

    def remote(src, dst, ssem, rsem, dev):
        return pltpu.make_async_remote_copy(src_ref=src, dst_ref=dst, send_sem=ssem, recv_sem=rsem, device_id=dev, device_id_type=MESH)

    def h_in(s):
        return pltpu.make_async_copy(h_hbm.at[s // nown, s % nown], hbuf.at[s], h_sem.at[s])

    @pl.loop(0, emb * nown)
    def _(s):
        h_in(s).start()

    @pl.loop(0, emb * nown)
    def _(s):
        h_in(s).wait()
        acc = jnp.zeros((seq, 128), F32)
        for n in range(width // 128):
            piece = hbuf[s, :, 128 * n : 128 * (n + 1)].astype(F32)
            acc += piece * piece
        ssum[s // 8, pl.ds(s % 8, 1), :] = jnp.sum(acc.T, axis=0, keepdims=True)

    pl.semaphore_wait(barrier, 6)

    def stat(k, dev):
        return remote(ssum, peers.at[k], p_snd.at[k], p_rcv.at[k], dev)

    stats = (stat(0, to_up), stat(1, to_down), stat(2, to_far))
    for cp in stats:
        cp.start()
    for cp in stats:
        cp.wait_recv()

    def far_up(u):
        return remote(pall.at[u, y_far, pl.ds(0, hr)], r2p.at[u], y_snd.at[0, u], y_rcv.at[0, u], to_up)

    def far_down(u):
        return remote(pall.at[u, y_far, pl.ds(hr, hr)], r2m.at[u], y_snd.at[1, u], y_rcv.at[1, u], to_down)

    def near_up(u):
        return remote(pall.at[u, y_next], r1p.at[u], y_snd.at[2, u], y_rcv.at[2, u], to_up)

    def near_down(u):
        return remote(pall.at[u, y_prev], r1m.at[u], y_snd.at[3, u], y_rcv.at[3, u], to_down)

    def local(u, k):
        return pltpu.make_async_copy(fin.at[u], own_hbm.at[u] if k else lat_hbm.at[j, u], g_snd.at[3 + k, u])

    def gather(u, owner, k, dev):
        return remote(fin.at[u], lat_hbm.at[owner, u], g_snd.at[k, u], g_rcv.at[k, u], dev)

    def relay(u, owner, lo, n, k, dev):
        part = lat_hbm.at[owner, u, pl.ds(lo, n), :]
        return remote(part, part, q_snd.at[k, u], q_rcv.at[k, u], dev)

    own_next, own_prev, own_far = 2 * x_next + c, 2 * x_prev + c, 2 * x_far + c
    sib = 1 - 2 * c
    nt = (((1,), (1,)), ((), ()))

    def stage_a(u):
        @pl.loop(0, emb)
        def _(yy):
            s = yy * nown + u
            ss = ssum[s // 8, pl.ds(s % 8, 1), :]
            for k in range(3):
                ss = ss + peers[k, s // 8, pl.ds(s % 8, 1), :]
            r_row = lax.rsqrt(ss / full_width + NORM_EPS)
            r = jnp.broadcast_to(r_row, (128, seq)).T
            hn = []
            for n in range(width // 128):
                piece = hbuf[s, :, 128 * n : 128 * (n + 1)].astype(F32)
                hn.append((piece * r * g_ref[:, 128 * n : 128 * (n + 1)].astype(F32)).astype(BF16))
            hn = jnp.concatenate(hn, axis=-1)
            hbuf[s] = hn
            pall[u, yy, pl.ds(0, seq), :] = lax.dot_general(hn, w_ref[pl.ds(0, lat_w), :], nt, preferred_element_type=F32).astype(BF16)
            mine = hbuf[s, pl.ds(j * sub, sub), :]
            kr = lax.dot_general(mine, w_ref[pl.ds(lat_w, 2 * kr_w), :], nt, preferred_element_type=F32).astype(BF16)
            pall[u, yy, pl.ds(seq, sub), pl.ds(0, 2 * kr_w)] = kr
            pall[u, yy, pl.ds(seq, sub), pl.ds(2 * kr_w, 2 * kr_w)] = jnp.zeros_like(kr)

        far_up(u).start()
        far_down(u).start()

    def stage_b(u):
        far_up(u).wait_recv()
        pall[u, y_next, pl.ds(0, hr)] = (pall[u, y_next, pl.ds(0, hr)].astype(F32) + r2p[u].astype(F32)).astype(BF16)
        near_up(u).start()
        far_down(u).wait_recv()
        pall[u, y_prev, pl.ds(hr, hr)] = (pall[u, y_prev, pl.ds(hr, hr)].astype(F32) + r2m[u].astype(F32)).astype(BF16)
        near_down(u).start()

    def stage_c(u):
        near_up(u).wait_recv()
        near_down(u).wait_recv()
        fin[u] = (pall[u, y].astype(F32) + r1p[u].astype(F32) + r1m[u].astype(F32)).astype(BF16)
        fin[u, pl.ds(seq, sub), pl.ds(2 * kr_w, 2 * kr_w)] = gains_ref[...]
        gather(u, j, 0, to_next).start()
        gather(u, j, 1, to_prev).start()
        gather(u, j, 2, to_sib).start()
        local(u, 0).start()
        local(u, 1).start()

    def stage_d(u):
        gather(u, own_prev, 0, to_next).wait_recv()
        relay(u, own_prev, 0, hr, 0, to_next).start()
        relay(u, own_prev, 0, ext, 2, to_sib).start()
        gather(u, own_next, 1, to_prev).wait_recv()
        relay(u, own_next, hr, hr, 1, to_prev).start()
        relay(u, own_next, 0, ext, 3, to_sib).start()

    def stage_e(u):
        relay(u, own_far, 0, hr, 0, to_next).wait_recv()
        relay(u, own_far, 0, hr, 4, to_sib).start()
        relay(u, own_far, hr, hr, 1, to_prev).wait_recv()
        relay(u, own_far, hr, hr, 5, to_sib).start()

    stages = (stage_a, stage_b, stage_c, stage_d, stage_e)

    @pl.loop(0, units + len(stages) - 1)
    def _(t):
        for lag, stage in enumerate(stages):

            @pl.when((t >= lag) & (t < units + lag))
            def _():
                stage(t - lag)

    @pl.loop(0, units)
    def _(u):
        for cp in (far_up, far_down, near_up, near_down):
            cp(u).wait_send()
        local(u, 0).wait()
        local(u, 1).wait()
        gather(u, j, 0, to_next).wait_send()
        gather(u, j, 1, to_prev).wait_send()
        gather(u, j, 2, to_sib).wait_send()
        relay(u, own_prev, 0, hr, 0, to_next).wait_send()
        relay(u, own_next, hr, hr, 1, to_prev).wait_send()
        relay(u, own_prev, 0, ext, 2, to_sib).wait_send()
        relay(u, own_next, 0, ext, 3, to_sib).wait_send()
        relay(u, own_far, 0, hr, 4, to_sib).wait_send()
        relay(u, own_far, hr, hr, 5, to_sib).wait_send()
        gather(u, j + sib, 2, to_sib).wait_recv()
        relay(u, own_prev + sib, 0, ext, 2, to_sib).wait_recv()
        relay(u, own_next + sib, 0, ext, 3, to_sib).wait_recv()
        relay(u, own_far + sib, 0, hr, 4, to_sib).wait_recv()
        relay(u, own_far + sib, hr, hr, 5, to_sib).wait_recv()

    for cp in stats:
        cp.wait_send()


def latents(h4, g_in, w_t, gains, cq_w, ckv_w, kr_w):
    emb, nseq, seq, width = h4.shape
    lat_w = cq_w + ckv_w
    assert emb == 4 and nseq == 8 and lat_w == 4 * kr_w
    ext = seq + seq // nseq
    dma = pltpu.SemaphoreType.DMA
    vm = pl.BlockSpec(memory_space=pltpu.VMEM)
    hbm = pl.BlockSpec(memory_space=pl.ANY)
    return pl.pallas_call(
        functools.partial(latent_kernel, cq_w, ckv_w, kr_w, width * emb),
        out_shape=[jax.ShapeDtypeStruct((nseq, nseq, ext, lat_w), BF16), jax.ShapeDtypeStruct((nseq, ext, lat_w), BF16)],
        in_specs=[hbm, vm, vm, vm],
        out_specs=[hbm, hbm],
        scratch_shapes=[
            pltpu.VMEM((emb * nseq, seq, width), BF16),
            pltpu.VMEM((emb * nseq // 8, 8, seq), F32),
            pltpu.VMEM((3, emb * nseq // 8, 8, seq), F32),
            pltpu.VMEM((nseq, emb, ext, lat_w), BF16),
            pltpu.VMEM((nseq, ext // 2, lat_w), BF16),
            pltpu.VMEM((nseq, ext // 2, lat_w), BF16),
            pltpu.VMEM((nseq, ext, lat_w), BF16),
            pltpu.VMEM((nseq, ext, lat_w), BF16),
            pltpu.VMEM((nseq, ext, lat_w), BF16),
            dma((emb * nseq,)), dma((3,)), dma((3,)),
            dma((4, nseq)), dma((4, nseq)),
            dma((5, nseq)), dma((3, nseq)),
            dma((6, nseq)), dma((6, nseq)),
        ],
        compiler_params=pltpu.CompilerParams(collective_id=1, has_side_effects=True, vmem_limit_bytes=60 * 1024 * 1024),
        cost_estimate=pl.CostEstimate(flops=2 * emb * nseq * seq * width * lat_w, bytes_accessed=2 * emb * nseq * seq * width, transcendentals=0),
        name="mla_latents",
    )(h4, g_in, w_t, gains)


def solution(mesh):
    emb_count = mesh.shape["emb"]
    in_specs = (P("dp", None, "emb"), P("emb"), P("emb", "head"), P("head"), P("emb", "head"), P("head"), P("emb", None), P(None, "head", None), P(None, "head", None), P(None, "head", None), P("head", None, "emb"))
    out_specs = (P("dp", None, "emb"), P("dp", None, "head"), P("dp", None, None))

    def local_block(hidden, g_in, w_dq, g_q, w_dkv, g_kv, w_kr, w_uq, w_uk, w_uv, w_o):
        batch, seq, width = hidden.shape
        nope, rope = w_uk.shape[2], w_kr.shape[1]
        heads = w_uq.shape[1]
        cq_w, ckv_w = w_dq.shape[1], w_dkv.shape[1]
        scale = MSCALE * MSCALE / math.sqrt(w_uq.shape[2])
        w_t = jnp.concatenate([w_dq.T, w_dkv.T, w_kr.T, w_kr.T], axis=0)
        g_loc = jnp.concatenate([g_q, g_kv]).reshape(2, 2 * rope)
        gains = jnp.pad(g_loc, ((0, seq // (batch // emb_count) - 2), (0, 0)))
        h4 = hidden.reshape(emb_count, batch // emb_count, seq, width)
        lat, own = latents(h4, g_in[None], w_t, gains, cq_w, ckv_w, rope)
        weights = (
            w_uq.transpose(1, 2, 0).reshape(-1, w_uq.shape[0]),
            w_uk.reshape(w_uk.shape[0], heads * nope),
            w_uv.reshape(w_uv.shape[0], -1),
        )
        o, small = attention(lat, own, weights, g_kv[None], rope_rows(seq, rope), scale, heads, rope, cq_w)
        result, small_all = tail(o, w_o.reshape(-1, w_o.shape[2]), hidden, small, emb_count)
        return result, small_all[:, :ckv_w].transpose(0, 2, 1), small_all[:, ckv_w:].transpose(0, 2, 1)

    return jax.shard_map(local_block, mesh=mesh, in_specs=in_specs, out_specs=out_specs, check_vma=False)
```
